32 devices in a mesh: expert: 8 (over y, x, core), hidden: 4 (over z).
Axes of the slice: x: 2, y: 2, z: 4, core: 2. Of those that a mesh axis runs over, the one named last changes fastest.
Arguments:
- weight: bfloat16 [8, 1536, 4096], P('expert', 'hidden'), may hold values from -0.15625 to 0.15625
- scales: float32 [8, 12, 32], P('expert'), may hold values from 0.5 to 2
- act_own: bfloat16 [8, 128, 1536], P('expert', None, 'hidden'), may hold values from -6 to 6
- dy_own: bfloat16 [8, 128, 4096], P('expert'), may hold values from -6 to 6
- own_count: int32 [8], P('expert'), may hold values from 1 to 128, as said below
- act_help: bfloat16 [8, 32, 1536], P('expert', None, 'hidden'), may hold values from -6 to 6
- dy_help: bfloat16 [8, 32, 4096], P('expert'), may hold values from -6 to 6
- help_count: int32 [8], P('expert'), may hold values from 1 to 32, as said below
- hot: int32 [1], replicated, may hold values from 0 to 7
Outputs:
- y_own: bfloat16 [8, 128, 4096], P('expert', None, 'hidden')
- dact_own: bfloat16 [8, 128, 1536], P('expert', None, 'hidden')
- own_grad: bfloat16 [8, 1536, 4096], P('expert', 'hidden')
- y_help: bfloat16 [8, 32, 4096], P('expert', None, 'hidden')
- dact_help: bfloat16 [8, 32, 1536], P('expert', None, 'hidden')
- hot_grad: float32 [1536, 4096], P('hidden', 'expert')
The draws below stay inside these ranges and needn't reach their ends.
Inputs may be any that keep to these rules, and one draw needn't show every extreme that they name: `own_count`: some expert has exactly 128 live rows. `help_count`: some group has exactly 32 live rows.
All inputs are finite; a program needn't handle non-finite values.
Results may differ from the reference program's by a relative error of at most 0.013.
Values may be sent and summed in bfloat16 or wider, within the bound.
No kernel may reach another device: no remote copies, remote signals or barrier semaphores. Data moves between devices by JAX's collectives and lax.ppermute only.
A program may use at most 64 MiB of HBM per device.

```python
import math
import jax
import jax.numpy as jnp
from jax import lax

D = 4096
FF = 1536
ROWS = 128
HROWS = 32
EXPERTS = 8
GROUPS = 8
N_HIDDEN = 4


def draw_own_count(key, part):
    first = jax.random.fold_in(key, 11)
    second = jax.random.fold_in(key, 12)
    counts = jax.random.randint(first, (EXPERTS,), 1, ROWS + 1, dtype=jnp.int32)
    chosen = jax.random.randint(second, (), 0, EXPERTS, dtype=jnp.int32)
    return counts.at[chosen].set(ROWS)


def draw_help_count(key, part):
    first = jax.random.fold_in(key, 21)
    second = jax.random.fold_in(key, 22)
    counts = jax.random.randint(first, (GROUPS,), 1, HROWS + 1, dtype=jnp.int32)
    chosen = jax.random.randint(second, (), 0, GROUPS, dtype=jnp.int32)
    return counts.at[chosen].set(HROWS)


def raised(array, key, source, target, blocks, factor):
    owner, partner = [(jnp.arange(array.shape[dim]) // (array.shape[dim] // blocks)).reshape([-1 if axis == dim else 1 for axis in range(array.ndim)]) for dim in (source, target)]
    chosen = jax.random.permutation(key, blocks)[partner]
    strong = (owner == chosen) | (owner == (partner + blocks // 2) % blocks)
    return jnp.where(strong, factor * array, array)


def block_levels(key, dims, cuts, least, high):
    gain = 1.0
    for axis_at, parts in cuts:
        heights = jax.random.uniform(jax.random.fold_in(jax.random.fold_in(key, 6), axis_at), (parts,), jnp.float32, least / len(cuts), high / len(cuts))
        gain = gain * jnp.repeat(jnp.exp(heights), dims[axis_at] // parts).reshape((-1,) + (1,) * (len(dims) - 1 - axis_at))
    return gain


def noise(key, dims, spread, limit, split=(), kind=jnp.bfloat16):
    values = jax.random.normal(key, dims, jnp.float32) * spread
    if len(split) > 0:
        values = block_levels(key, dims, split, -0.22, 0.18) * values
    return jnp.clip(values, min=-limit, max=limit).astype(kind)


def noise_with(rng, shape, scale, most, cuts, heavy, held_as=jnp.bfloat16):
    result = scale * jax.random.normal(rng, shape, jnp.float32)
    if cuts:
        result = result * block_levels(rng, shape, cuts, -0.22, 0.18)
    return jnp.clip(raised(result, jax.random.fold_in(rng, 3), *heavy), -most, most).astype(held_as)


def setup_inputs(seed: int = 0) -> dict:
    splits = jax.random.split(jax.random.key(seed), 10)
    return {
        "weight": noise(splits[0], (EXPERTS, FF, D), FF ** -0.5, 0.15625, ((0, 8), (1, 4))),
        "scales": jnp.clip(jnp.exp(math.log(2.0) - 1.3862944 * jax.random.uniform(splits[1], (EXPERTS, FF // 128, D // 128), jnp.float32) ** block_levels(splits[1], (EXPERTS, FF // 128, D // 128), ((0, 8),), -0.2, 0.2)), 0.5, 2.0),
        "act_own": noise(splits[2], (EXPERTS, ROWS, FF), 1.0, 6.0, ((0, 8), (2, 4))),
        "dy_own": noise(splits[3], (EXPERTS, ROWS, D), 1.0, 6.0, ((0, 8),)),
        "own_count": draw_own_count(jax.random.fold_in(splits[9], 71), 0),
        "act_help": noise(splits[5], (GROUPS, HROWS, FF), 1.0, 6.0, ((0, 8), (2, 4))),
        "dy_help": noise_with(splits[6], (GROUPS, HROWS, D), 1.0, 6.0, ((0, 8),), (0, 2, 8, 2.0)),
        "help_count": draw_help_count(jax.random.fold_in(splits[9], 71), 0),
        "hot": jax.random.randint(splits[8], (1,), 0, EXPERTS).astype(jnp.int32),
    }


def dequant(weight, scales):
    full = jnp.repeat(jnp.repeat(scales, 128, axis=0), 128, axis=1)
    return (weight.astype(jnp.float32) * full).astype(jnp.bfloat16)


def masked(values, count):
    live = jnp.arange(values.shape[0], dtype=jnp.int32)[:, None] < count
    return jnp.where(live, values, jnp.zeros_like(values))


def forward_back(weight_deq, rows, grads):
    nrows = rows.shape[0]
    wide = weight_deq.astype(jnp.float32)
    pieces = rows.astype(jnp.float32).reshape(nrows, N_HIDDEN, FF // N_HIDDEN)
    slices = wide.reshape(N_HIDDEN, FF // N_HIDDEN, D)
    partial_value = jnp.einsum("rhf,hfd->hrd", pieces, slices).astype(jnp.bfloat16)
    partial_value = lax.optimization_barrier(partial_value)
    outputs = jnp.sum(partial_value.astype(jnp.float32), axis=0).astype(jnp.bfloat16)
    grads_wide = grads.astype(jnp.float32)
    dact = jnp.einsum("rd,fd->rf", grads_wide, wide).astype(jnp.bfloat16)
    gradient = jnp.einsum("rf,rd->fd", rows.astype(jnp.float32), grads_wide)
    return outputs, dact, gradient


def reference(weight, scales, act_own, dy_own, own_count, act_help, dy_help, help_count, hot):
    def own_expert(items):
        raw, block_scales, rows, grads, count = items
        weight_deq = dequant(raw, block_scales)
        outputs, dact, gradient = forward_back(weight_deq, masked(rows, count), masked(grads, count))
        return outputs, dact, gradient.astype(jnp.bfloat16)

    y_own, dact_own, own_grad = lax.map(own_expert, (weight, scales, act_own, dy_own, own_count))
    hot_index = hot[0].astype(jnp.int32)
    hot_raw = lax.dynamic_index_in_dim(weight, hot_index, 0, keepdims=False)
    hot_scales = lax.dynamic_index_in_dim(scales, hot_index, 0, keepdims=False)
    hot_weight = dequant(hot_raw, hot_scales)

    def one_group(total, items):
        rows, grads, count = items
        outputs, dact, gradient = forward_back(hot_weight, masked(rows, count), masked(grads, count))
        return total + gradient, (outputs, dact)

    start_total = jnp.zeros((FF, D), jnp.float32)
    hot_grad, (y_help, dact_help) = lax.scan(one_group, start_total, (act_help, dy_help, help_count))
    return y_own, dact_own, own_grad, y_help, dact_help, hot_grad
```

```python
import functools

import jax
import jax.numpy as jnp
from jax import lax
from jax.experimental import pallas as pl
from jax.experimental.pallas import tpu as pltpu
from jax.sharding import PartitionSpec as P

block_edge = 128


def from_root(block, axis, source):
    block = jnp.where(lax.axis_index(axis) == source, block, jnp.zeros_like(block))
    return lax.psum(block, axis)


def dequant(weight, scales, slice_start):
    height = weight.shape[1]
    depth = weight.shape[2]
    blocks = (slice_start + jnp.arange(height, dtype=jnp.int32)) // block_edge
    select = (blocks[:, None] == jnp.arange(scales.shape[1], dtype=jnp.int32)[None, :]).astype(
        jnp.float32
    )
    row_scale = jnp.einsum("fb,ebc->efc", select, scales, precision=lax.Precision.HIGHEST)
    shaped = weight.reshape(weight.shape[0], height, depth // block_edge, block_edge).astype(
        jnp.float32
    )
    shaped = shaped * row_scale[..., None]
    return shaped.reshape(weight.shape).astype(jnp.bfloat16)


def masked(values, count):
    live = jnp.arange(values.shape[1], dtype=jnp.int32)[None, :, None] < count[:, None, None]
    return jnp.where(live, values, jnp.zeros_like(values))


def weights_to_rows(weight, scales, act_own, dy_own, own_count, act_help, dy_help, help_count, hot):
    slice_start = lax.axis_index("hidden") * weight.shape[1]
    own_weight = dequant(weight, scales, slice_start)
    experts_here = weight.shape[0]
    hot_index = hot[0]
    hot_local = hot_index % experts_here
    hot_root = hot_index // experts_here
    own_rows = masked(act_own, own_count)
    own_grads = masked(dy_own, own_count)
    help_rows = masked(act_help, help_count)[0]
    help_grads = masked(dy_help, help_count)[0]
    partial_value = jnp.einsum(
        "erf,efd->erd", own_rows, own_weight, preferred_element_type=jnp.float32
    )
    dact = jnp.einsum("erd,efd->erf", own_grads, own_weight, preferred_element_type=jnp.float32)
    gradient = jnp.einsum("erf,erd->efd", own_rows, own_grads, preferred_element_type=jnp.float32)
    dact_own = dact.astype(jnp.bfloat16)
    own_grad = gradient.astype(jnp.bfloat16)
    chosen = lax.dynamic_index_in_dim(own_weight, hot_local, 0, keepdims=False)
    hot_weight = from_root(chosen, "expert", hot_root)
    help_partial_value = jnp.dot(help_rows, hot_weight, preferred_element_type=jnp.float32)
    dact = lax.dot_general(
        help_grads, hot_weight, (((1,), (1,)), ((), ())), preferred_element_type=jnp.float32
    )
    gradient = lax.dot_general(
        help_rows, help_grads, (((0,), (0,)), ((), ())), preferred_element_type=jnp.float32
    )
    summed = lax.psum_scatter(gradient, "expert", scatter_dimension=1, tiled=True)
    help_partial = help_partial_value[None]
    dact_help = dact.astype(jnp.bfloat16)[None]
    y_own, y_help = (
        lax.psum_scatter(
            partial_value.astype(jnp.bfloat16), "hidden", scatter_dimension=2, tiled=True
        ).astype(jnp.float32),
        lax.psum_scatter(
            help_partial.astype(jnp.bfloat16), "hidden", scatter_dimension=2, tiled=True
        ).astype(jnp.float32),
    )
    return (
        y_own.astype(jnp.bfloat16),
        dact_own,
        own_grad,
        y_help.astype(jnp.bfloat16),
        dact_help,
        summed,
    )


def scale_kernel(scale_ref, weight_ref, rows_ref, count_ref, scaled_ref, value_ref):
    step = pl.program_id(0)
    height, width = weight_ref.shape
    across = width // block_edge
    for column in range(across):
        cols = pl.ds(column * block_edge, block_edge)
        for row in range(height // block_edge):
            part = pl.ds(row * block_edge, block_edge)
            scale = scale_ref[row, step * across + column]
            scaled_ref[part, cols] = (weight_ref[part, cols].astype(jnp.float32) * scale).astype(
                scaled_ref.dtype
            )
    live = lax.broadcasted_iota(jnp.int32, rows_ref.shape, 0) < count_ref[0]
    rows = jnp.where(live, rows_ref[...], jnp.zeros_like(rows_ref))
    value_ref[0] = jnp.dot(rows, scaled_ref[...], preferred_element_type=jnp.float32).astype(
        value_ref.dtype
    )


def scale_and_forward(weight, scales, rows, count, pieces):
    height, depth = weight.shape
    width = depth // pieces
    nrows = rows.shape[0]
    return pl.pallas_call(
        scale_kernel,
        grid=(pieces,),
        in_specs=[
            pl.BlockSpec(memory_space=pltpu.SMEM),
            pl.BlockSpec((height, width), lambda i: (0, i)),
            pl.BlockSpec((nrows, height), lambda i: (0, 0)),
            pl.BlockSpec(memory_space=pltpu.SMEM),
        ],
        out_specs=[
            pl.BlockSpec((height, width), lambda i: (0, i)),
            pl.BlockSpec((1, nrows, width), lambda i: (i, 0, 0)),
        ],
        out_shape=[
            jax.ShapeDtypeStruct((height, depth), jnp.bfloat16),
            jax.ShapeDtypeStruct((pieces, nrows, width), jnp.bfloat16),
        ],
        cost_estimate=pl.CostEstimate(
            flops=2 * nrows * height * depth,
            bytes_accessed=4 * height * depth + 2 * nrows * (height + depth),
            transcendentals=0,
        ),
        name="scale_and_forward",
    )(scales, weight, rows, count)


def swap(block, axis, size, mask):
    return lax.ppermute(block, axis, [(i, i ^ mask) for i in range(size)])


def hidden_sum(pieces, size):
    if size == 1:
        return pieces[0]
    if size == 2:
        near = swap(pieces[1], "hidden", size, 1)
        return (pieces[0].astype(jnp.float32) + near.astype(jnp.float32)).astype(jnp.bfloat16)
    far_half = swap(pieces[3], "hidden", size, 1)
    near = swap(pieces[1], "hidden", size, 1)
    pair = (pieces[2].astype(jnp.float32) + far_half.astype(jnp.float32)).astype(jnp.bfloat16)
    far = swap(pair, "hidden", size, 2)
    return (
        pieces[0].astype(jnp.float32) + near.astype(jnp.float32) + far.astype(jnp.float32)
    ).astype(jnp.bfloat16)


def pick(options, index):
    chosen = options[0]
    for k in range(1, len(options)):
        chosen = jnp.where(index == k, options[k], chosen)
    return chosen


def relative(stacked, index, size):
    return [lax.dynamic_index_in_dim(stacked, index ^ k, 0, keepdims=False) for k in range(size)]


def rows_to_owner(
    groups, slices, weight, scales, act_own, dy_own, own_count, act_help, dy_help, help_count, hot
):
    height, depth = weight.shape[1:]
    chips = groups // 2
    me = lax.axis_index("expert")
    place = lax.axis_index("hidden")
    hot_index = hot[0]

    help_rows = masked(act_help, help_count)[0]
    help_grads = masked(dy_help, help_count)[0]
    rows_same = [help_rows] + [swap(help_rows, "expert", groups, 2 * k) for k in range(1, chips)]
    rows_same = jnp.concatenate(rows_same, axis=0)
    rows_other = swap(rows_same, "expert", groups, 1)
    grads_same = [help_grads] + [swap(help_grads, "expert", groups, 2 * k) for k in range(1, chips)]
    grads_same = jnp.concatenate(grads_same, axis=0)
    grads_other = swap(grads_same, "expert", groups, 1)

    tall = height // block_edge
    here = lax.dynamic_slice_in_dim(scales[0], place * tall, tall, 0)
    own_weight, own_value = scale_and_forward(weight[0], here, act_own[0], own_count, slices)
    y_own = hidden_sum(relative(own_value, place, slices), slices)

    own_rows = masked(act_own, own_count)[0]
    own_grads = masked(dy_own, own_count)[0]
    by_weight = (((1,), (1,)), ((), ()))
    by_row = (((0,), (0,)), ((), ()))
    dact_own = lax.dot_general(
        own_grads, own_weight, by_weight, preferred_element_type=jnp.float32
    ).astype(jnp.bfloat16)
    own_grad = lax.dot_general(
        own_rows, own_grads, by_row, preferred_element_type=jnp.float32
    ).astype(jnp.bfloat16)

    mine = me % 2 == hot_index % 2
    away = (hot_index // 2) ^ (me // 2)
    each = help_rows.shape[0]

    def send_back(same, other):
        other = swap(other, "expert", groups, 1)
        same = jnp.where(mine, same, other)
        parts = [same[k * each : (k + 1) * each] for k in range(chips)]
        back = [parts[0]] + [swap(parts[k], "expert", groups, 2 * k) for k in range(1, chips)]
        return pick(back, away)

    def forward(rows):
        return jnp.dot(rows, own_weight, preferred_element_type=jnp.float32).astype(jnp.bfloat16)

    def backward(grads):
        return lax.dot_general(
            grads, own_weight, by_weight, preferred_element_type=jnp.float32
        ).astype(jnp.bfloat16)

    help_value = send_back(forward(rows_same), forward(rows_other))
    help_value = jnp.transpose(help_value.reshape(each, slices, depth // slices), (1, 0, 2))
    y_help = hidden_sum(relative(help_value, place, slices), slices)
    dact_help = send_back(backward(grads_same), backward(grads_other))

    wide = depth // groups
    columns = jnp.concatenate(
        [
            lax.dynamic_slice_in_dim(grads_same, me * wide, wide, 1),
            lax.dynamic_slice_in_dim(grads_other, me * wide, wide, 1),
        ],
        axis=0,
    )
    hot_grad = lax.dot_general(
        jnp.concatenate([rows_same, rows_other], axis=0),
        columns,
        by_row,
        preferred_element_type=jnp.float32,
    )
    return y_own[None], dact_own[None], own_grad[None], y_help[None], dact_help[None], hot_grad


def solution(mesh):
    groups, slices = mesh.shape["expert"], mesh.shape["hidden"]

    def body(weight, scales, act_own, dy_own, own_count, act_help, dy_help, help_count, hot):
        args = (weight, scales, act_own, dy_own, own_count, act_help, dy_help, help_count, hot)
        experts, height, depth = weight.shape
        few = groups * act_help.shape[1] <= 2 * height and groups in (2, 4, 8, 16)
        even = height % block_edge == 0 and depth % (groups * block_edge) == 0
        if experts == 1 and few and even and slices in (1, 2, 4):
            return rows_to_owner(groups, slices, *args)
        return weights_to_rows(*args)

    return jax.shard_map(
        body,
        mesh=mesh,
        in_specs=(
            P("expert", "hidden", None),
            P("expert", None, None),
            P("expert", None, "hidden"),
            P("expert", None, None),
            P("expert"),
            P("expert", None, "hidden"),
            P("expert", None, None),
            P("expert"),
            P(),
        ),
        out_specs=(
            P("expert", None, "hidden"),
            P("expert", None, "hidden"),
            P("expert", "hidden", None),
            P("expert", None, "hidden"),
            P("expert", None, "hidden"),
            P("hidden", "expert"),
        ),
        check_vma=False,
    )
```

```python
import functools

import jax
import jax.numpy as jnp
from jax import lax
from jax.experimental import pallas as pl
from jax.experimental.pallas import tpu as pltpu
from jax.sharding import PartitionSpec as P


block_edge = 128


def from_root(block, axis, source):
    block = jnp.where(lax.axis_index(axis) == source, block, jnp.zeros_like(block))
    return lax.psum(block, axis)


def dequant(weight, scales, slice_start):
    height = weight.shape[1]
    depth = weight.shape[2]
    blocks = (slice_start + jnp.arange(height, dtype=jnp.int32)) // block_edge
    select = (blocks[:, None] == jnp.arange(scales.shape[1], dtype=jnp.int32)[None, :]).astype(
        jnp.float32
    )
    row_scale = jnp.einsum("fb,ebc->efc", select, scales, precision=lax.Precision.HIGHEST)
    shaped = weight.reshape(weight.shape[0], height, depth // block_edge, block_edge).astype(
        jnp.float32
    )
    shaped = shaped * row_scale[..., None]
    return shaped.reshape(weight.shape).astype(jnp.bfloat16)


def masked(values, count):
    live = jnp.arange(values.shape[1], dtype=jnp.int32)[None, :, None] < count[:, None, None]
    return jnp.where(live, values, jnp.zeros_like(values))


def weights_to_rows(weight, scales, act_own, dy_own, own_count, act_help, dy_help, help_count, hot):
    slice_start = lax.axis_index("hidden") * weight.shape[1]
    own_weight = dequant(weight, scales, slice_start)
    experts_here = weight.shape[0]
    hot_index = hot[0]
    hot_local = hot_index % experts_here
    hot_root = hot_index // experts_here
    own_rows = masked(act_own, own_count)
    own_grads = masked(dy_own, own_count)
    help_rows = masked(act_help, help_count)[0]
    help_grads = masked(dy_help, help_count)[0]
    partial_value = jnp.einsum(
        "erf,efd->erd", own_rows, own_weight, preferred_element_type=jnp.float32
    )
    dact = jnp.einsum("erd,efd->erf", own_grads, own_weight, preferred_element_type=jnp.float32)
    gradient = jnp.einsum("erf,erd->efd", own_rows, own_grads, preferred_element_type=jnp.float32)
    dact_own = dact.astype(jnp.bfloat16)
    own_grad = gradient.astype(jnp.bfloat16)
    chosen = lax.dynamic_index_in_dim(own_weight, hot_local, 0, keepdims=False)
    hot_weight = from_root(chosen, "expert", hot_root)
    help_partial_value = jnp.dot(help_rows, hot_weight, preferred_element_type=jnp.float32)
    dact = lax.dot_general(
        help_grads, hot_weight, (((1,), (1,)), ((), ())), preferred_element_type=jnp.float32
    )
    gradient = lax.dot_general(
        help_rows, help_grads, (((0,), (0,)), ((), ())), preferred_element_type=jnp.float32
    )
    summed = lax.psum_scatter(gradient, "expert", scatter_dimension=1, tiled=True)
    help_partial = help_partial_value[None]
    dact_help = dact.astype(jnp.bfloat16)[None]
    y_own, y_help = (
        lax.psum_scatter(
            partial_value.astype(jnp.bfloat16), "hidden", scatter_dimension=2, tiled=True
        ).astype(jnp.float32),
        lax.psum_scatter(
            help_partial.astype(jnp.bfloat16), "hidden", scatter_dimension=2, tiled=True
        ).astype(jnp.float32),
    )
    return (
        y_own.astype(jnp.bfloat16),
        dact_own,
        own_grad,
        y_help.astype(jnp.bfloat16),
        dact_help,
        summed,
    )


by_weight = (((1,), (1,)), ((), ()))
by_row = (((0,), (0,)), ((), ()))


def product(left, right, dims=(((1,), (0,)), ((), ()))):
    return lax.dot_general(left, right, dims, preferred_element_type=jnp.float32)


def live_rows(values, count):
    live = lax.broadcasted_iota(jnp.int32, values.shape, 0) < count
    return jnp.where(live, values, jnp.zeros_like(values))


def scale_into(stored, weight_ref, scale_of, first):
    height, width = weight_ref.shape
    for column in range(width // block_edge):
        cols = slice(column * block_edge, (column + 1) * block_edge)
        for row in range(height // block_edge):
            part = slice(row * block_edge, (row + 1) * block_edge)
            stored[part, cols] = (
                weight_ref[part, cols].astype(jnp.float32) * scale_of(row, first + column)
            ).astype(jnp.bfloat16)


def pick_into(stored, mine, own_ref, other_ref, scale_of, first):
    height, width = own_ref.shape
    for column in range(width // block_edge):
        cols = slice(column * block_edge, (column + 1) * block_edge)
        for row in range(height // block_edge):
            part = slice(row * block_edge, (row + 1) * block_edge)
            block = jnp.where(mine, own_ref[part, cols], other_ref[part, cols])
            stored[part, cols] = (
                block.astype(jnp.float32) * scale_of(row, first + column)
            ).astype(jnp.bfloat16)


hbm_place = pl.BlockSpec(memory_space=pltpu.HBM)
smem_place = pl.BlockSpec(memory_space=pltpu.SMEM)
vmem_place = pl.BlockSpec(memory_space=pltpu.VMEM)
grant = pltpu.CompilerParams(vmem_limit_bytes=16 * 2**20)


def own_forward_kernel(pieces, scale_ref, count_ref, rows_ref, weight_ref, *refs):
    out_refs = refs[:pieces]
    (stored,) = refs[pieces:]
    height, depth = weight_ref.shape
    width = depth // pieces
    place = lax.axis_index("hidden")
    top = place * (height // block_edge)
    live = live_rows(rows_ref[...], count_ref[0])
    for i in range(pieces):
        start = pl.multiple_of((place ^ i) * width, width)
        block = weight_ref.at[:, pl.ds(start, width)]
        first = start // block_edge
        scale_into(stored.at[i % 2], block, lambda r, c: scale_ref[top + r, 0, c], first)
        out_refs[i][...] = product(live, stored[i % 2]).astype(jnp.bfloat16)


def own_forward(scales, weight, rows, count, pieces):
    height, depth = weight.shape
    nrows = rows.shape[0]
    width = depth // pieces
    return pl.pallas_call(
        functools.partial(own_forward_kernel, pieces),
        in_specs=[smem_place] * 2 + [vmem_place] * 2,
        out_specs=[vmem_place] * pieces,
        out_shape=[jax.ShapeDtypeStruct((nrows, width), jnp.bfloat16)] * pieces,
        scratch_shapes=[pltpu.VMEM((2, height, width), jnp.bfloat16)],
        compiler_params=grant,
        cost_estimate=pl.CostEstimate(
            flops=2 * nrows * height * depth,
            bytes_accessed=2 * height * depth + 2 * nrows * (height + depth),
            transcendentals=0,
        ),
        name="own_forward",
    )(scales, count, rows, weight)


def own_backward_kernel(scale_ref, count_ref, rows_ref, grads_ref, weight_ref, ours, theirs,
                        dact_ref, grad_ref, hot_ref, stored, made, dact, total, hot, out_sems, end_sems):
    height, _ = weight_ref.shape
    steps, _, width = made.shape
    top = lax.axis_index("hidden") * (height // block_edge)
    live = live_rows(rows_ref[...], count_ref[0])
    out = []
    for i in range(steps):
        cols = slice(i * width, (i + 1) * width)
        live_grads = live_rows(grads_ref[:, cols], count_ref[0])
        made[i] = product(live, live_grads, by_row).astype(jnp.bfloat16)
        out.append(pltpu.make_async_copy(made.at[i], grad_ref.at[:, cols], out_sems.at[i]))
        out[-1].start()
        first = i * (width // block_edge)
        scale_into(stored.at[i % 2], weight_ref.at[:, cols], lambda r, c: scale_ref[top + r, 0, c], first)
        part = product(live_grads, stored[i % 2], by_weight)
        total[...] = part if i == 0 else total[...] + part
    dact[...] = total[...].astype(jnp.bfloat16)
    out.append(pltpu.make_async_copy(dact, dact_ref, end_sems.at[0]))
    out[-1].start()
    hot[...] = product(ours[:, :height], ours[:, height:], by_row) + product(
        theirs[:, :height], theirs[:, height:], by_row
    )
    out.append(pltpu.make_async_copy(hot, hot_ref, end_sems.at[1]))
    out[-1].start()
    for copy in out:
        copy.wait()


def own_backward(scales, weight, rows, grads, count, ours, theirs):
    height, depth = weight.shape
    nrows = rows.shape[0]
    hrows, wide = ours.shape[0], ours.shape[1] - height
    width = 1024
    steps = depth // width
    return pl.pallas_call(
        own_backward_kernel,
        in_specs=[smem_place] * 2 + [vmem_place] * 5,
        out_specs=[hbm_place] * 3,
        out_shape=[
            jax.ShapeDtypeStruct((nrows, height), jnp.bfloat16),
            jax.ShapeDtypeStruct((height, depth), jnp.bfloat16),
            jax.ShapeDtypeStruct((height, wide), jnp.float32),
        ],
        scratch_shapes=[
            pltpu.VMEM((2, height, width), jnp.bfloat16),
            pltpu.VMEM((steps, height, width), jnp.bfloat16),
            pltpu.VMEM((nrows, height), jnp.bfloat16),
            pltpu.VMEM((nrows, height), jnp.float32),
            pltpu.VMEM((height, wide), jnp.float32),
            pltpu.SemaphoreType.DMA((steps,)),
            pltpu.SemaphoreType.DMA((2,)),
        ],
        compiler_params=grant,
        cost_estimate=pl.CostEstimate(
            flops=4 * nrows * height * depth + 4 * hrows * height * wide,
            bytes_accessed=4 * height * depth + 4 * nrows * (height + depth) + 4 * height * wide,
            transcendentals=0,
        ),
        name="own_backward",
    )(scales, count, rows, grads, weight, ours, theirs)


def help_kernel(count, pieces, wide, hot_ref, scale_ref, other_scale_ref, own_ref, other_ref, *refs):
    in_refs, out_refs = refs[:count], refs[count : 2 * count]
    ours_ref, theirs_ref = refs[2 * count : 2 * count + 2]
    stored, total = refs[2 * count + 2 :]
    height, depth = own_ref.shape
    width = depth // pieces
    me, place = lax.axis_index("expert"), lax.axis_index("hidden")
    mine = me % 2 == hot_ref[0] % 2
    top = place * (height // block_edge)
    each = in_refs[0].shape[0]
    starts = [pl.multiple_of((place ^ piece) * width, width) for piece in range(pieces)]

    def rows(cols):
        return jnp.concatenate([ref[:, cols] for ref in in_refs], axis=0)

    def scale_of(row, column):
        return jnp.where(mine, scale_ref[top + row, 0, column], other_scale_ref[top + row, 0, column])

    acts = rows(slice(0, height))
    for ref, index in ((ours_ref, me), (theirs_ref, me ^ 1)):
        ref[:, :height] = acts
        ref[:, height:] = rows(pl.ds(pl.multiple_of(height + index * wide, block_edge), wide))
    for i in range(pieces):
        first = starts[i] // block_edge
        spot = stored.at[i % 2]
        cols = pl.ds(starts[i], width)
        pick_into(spot, mine, own_ref.at[:, cols], other_ref.at[:, cols], scale_of, first)
        value = product(acts, spot[...]).astype(jnp.bfloat16)
        for k, ref in enumerate(out_refs):
            ref[:, i * width : (i + 1) * width] = value[k * each : (k + 1) * each]
        grads = rows(pl.ds(pl.multiple_of(height + starts[i], block_edge), width))
        part = product(grads, spot[...], by_weight)
        total[...] = part if i == 0 else total[...] + part
    for k, ref in enumerate(out_refs):
        ref[:, depth:] = total[k * each : (k + 1) * each, :].astype(jnp.bfloat16)


def help_both(hot, scales, other_scales, weight, other_weight, rows, pieces, wide):
    height, depth = weight.shape
    count, each = len(rows), rows[0].shape[0]
    nrows = count * each
    width = depth // pieces
    shape = lambda r, c: jax.ShapeDtypeStruct((r, c), jnp.bfloat16)
    return pl.pallas_call(
        functools.partial(help_kernel, count, pieces, wide),
        in_specs=[smem_place] * 3 + [vmem_place] * (2 + count),
        out_specs=[vmem_place] * (count + 2),
        out_shape=[shape(each, depth + height)] * count + [shape(nrows, height + wide)] * 2,
        scratch_shapes=[
            pltpu.VMEM((2, height, width), jnp.bfloat16),
            pltpu.VMEM((nrows, height), jnp.float32),
        ],
        compiler_params=grant,
        cost_estimate=pl.CostEstimate(
            flops=4 * nrows * height * depth,
            bytes_accessed=2 * height * depth + 4 * nrows * (height + depth),
            transcendentals=0,
        ),
        name="help_both",
    )(hot, scales, other_scales, weight, other_weight, *rows)


def swap(block, axis, size, mask):
    return lax.ppermute(block, axis, [(i, i ^ mask) for i in range(size)])


def over_hidden(pieces, size):
    return [pieces[0]] + [swap(pieces[k], "hidden", size, k) for k in range(1, size)]


def add_up(parts):
    total = parts[0].astype(jnp.float32)
    for part in parts[1:]:
        total = total + part.astype(jnp.float32)
    return total.astype(jnp.bfloat16)


def pick(options, index):
    chosen = options[0]
    for k in range(1, len(options)):
        chosen = jnp.where(index == k, options[k], chosen)
    return chosen


def rows_to_owner(
    groups, slices, weight, scales, act_own, dy_own, own_count, act_help, dy_help, help_count, hot
):
    _, depth = weight.shape[1:]
    chips = groups // 2
    me = lax.axis_index("expert").astype(jnp.int32)
    away = (hot[0] // 2) ^ (me // 2)
    scales = jnp.transpose(scales, (1, 0, 2))
    other_scales = swap(scales, "expert", groups, 1)
    other_weight = swap(weight[0], "expert", groups, 1)

    def over_chips(parts):
        return [parts[0]] + [swap(parts[k], "expert", groups, 2 * k) for k in range(1, chips)]

    joined = jnp.concatenate([act_help, dy_help], axis=2)
    rows = over_chips([masked(joined, help_count)[0]] * chips)
    own_parts = over_hidden(own_forward(scales, weight[0], act_own[0], own_count, slices), slices)

    wide = depth // groups
    *results, ours, theirs = help_both(
        hot, scales, other_scales, weight[0], other_weight, rows, slices, wide
    )
    theirs = swap(theirs, "expert", groups, 1)
    result = pick(over_chips(results), away)
    width = depth // slices
    help_parts = over_hidden(
        [result[:, k * width : (k + 1) * width] for k in range(slices)], slices
    )
    y_help = add_up(help_parts)
    own_parts, _ = lax.optimization_barrier((own_parts, result))
    y_own = add_up(own_parts)
    dact_help = result[:, depth:]

    dact_own, own_grad, hot_grad = own_backward(
        scales, weight[0], act_own[0], dy_own[0], own_count, ours, theirs
    )
    return y_own[None], dact_own[None], own_grad[None], y_help[None], dact_help[None], hot_grad


def solution(mesh):
    groups, slices = mesh.shape["expert"], mesh.shape["hidden"]

    def body(weight, scales, act_own, dy_own, own_count, act_help, dy_help, help_count, hot):
        args = (weight, scales, act_own, dy_own, own_count, act_help, dy_help, help_count, hot)
        experts, height, depth = weight.shape
        few = groups * act_help.shape[1] <= 2 * height and groups in (2, 4, 8, 16)
        even = height % block_edge == 0 and depth % 1024 == 0
        even = even and depth % (groups * block_edge) == 0 and depth % (slices * 256) == 0
        if experts == 1 and few and even and slices in (2, 4, 8):
            return rows_to_owner(groups, slices, *args)
        return weights_to_rows(*args)

    return jax.shard_map(
        body,
        mesh=mesh,
        in_specs=(
            P("expert", "hidden", None),
            P("expert", None, None),
            P("expert", None, "hidden"),
            P("expert", None, None),
            P("expert"),
            P("expert", None, "hidden"),
            P("expert", None, None),
            P("expert"),
            P(),
        ),
        out_specs=(
            P("expert", None, "hidden"),
            P("expert", None, "hidden"),
            P("expert", "hidden", None),
            P("expert", None, "hidden"),
            P("expert", None, "hidden"),
            P("hidden", "expert"),
        ),
        check_vma=False,
    )
```
